32 devices in a mesh: shot: 2 (over x), slab: 16 (over z, y, core).
Axes of the slice: x: 2, y: 2, z: 4, core: 2. Of those that a mesh axis runs over, the one named last changes fastest.
Arguments:
- partial_grads: bfloat16 [2, 3, 1024, 32, 256], P('shot', None, 'slab'), may hold values from -6 to 6
- model: float32 [3, 1024, 32, 256], P(None, 'slab', 'shot'), may hold values from 0.8 to 1.6
- tilt: float32 [1024, 32, 256], P('slab', 'shot'), may hold values from -3.140625 to 3.140625
- widths: float32 [3, 1024], replicated, may hold values from 2 to 64
- step_length: float32 [3], replicated, may hold values from 0.1 to 0.4
Outputs:
- coefficients: float32 [3, 1024, 32, 256], P(None, 'slab', 'shot')
The draws below stay inside these ranges and needn't reach their ends.
All inputs are finite; a program needn't handle non-finite values.
Results may differ from the reference program's by a relative error of at most 0.004.
Values may be sent and summed in bfloat16 or wider, within the bound.
No kernel may reach another device: no remote copies, remote signals or barrier semaphores. Data moves between devices by JAX's collectives and lax.ppermute only.
A program may use at most 64 MiB of HBM per device.

```python
import math
import jax
import jax.numpy as jnp

NZ = 1024
NY = 256
NX = 32
N_SHOT = 2


def with_spikes(array, own_key, source, target, blocks, factor):
    owner, partner = [(jnp.arange(array.shape[dim]) // (array.shape[dim] // blocks)).reshape([-1 if axis == dim else 1 for axis in range(array.ndim)]) for dim in (source, target)]
    chosen = jax.random.permutation(own_key, blocks)[partner]
    strong = (owner == chosen) | (owner == (partner + blocks // 2) % blocks)
    return jnp.where(strong, factor * array, array)


def block_levels(rng, dims, pieces, least, top_value):
    def one(axis_at, parts):
        steps = jax.random.uniform(jax.random.fold_in(jax.random.fold_in(rng, 6), axis_at), (parts,), jnp.float32, least / len(pieces), top_value / len(pieces))
        return jnp.repeat(jnp.exp(steps), dims[axis_at] // parts).reshape((-1,) + (1,) * (len(dims) - axis_at - 1))

    gain = one(*pieces[0])
    for cut in pieces[1:]:
        gain = gain * one(*cut)
    return gain


def bell_draw_with(rng, shape, deviation, most, cuts, heavy, kind=jnp.bfloat16):
    values = deviation * jax.random.normal(rng, shape, jnp.float32)
    if cuts:
        values = values * block_levels(rng, shape, cuts, -0.22, 0.18)
    return jnp.clip(with_spikes(values, jax.random.fold_in(rng, 3), *heavy), -most, most).astype(kind)


def setup_inputs(seed: int = 0) -> dict:
    key_of = jax.random.split(jax.random.key(seed), 6)
    partial_grads = bell_draw_with(key_of[0], (N_SHOT, 3, NZ, NX, NY), 1.0, 6.0, ((0, 2), (2, 16)), (0, 3, 2, 2.0))
    model = jnp.clip(0.8 + 0.8 * jax.random.uniform(key_of[1], (3, NZ, NX, NY), jnp.float32) ** block_levels(key_of[1], (3, NZ, NX, NY), ((1, 16), (2, 2)), -0.2, 0.2), 0.8, 1.6)
    tilt = jnp.clip(jax.random.uniform(key_of[2], (NZ, NX, NY), jnp.float32, -3.140625, 3.140625), -3.140625, 3.140625)
    widths = jnp.clip(jnp.exp(jax.random.uniform(key_of[3], (3, NZ), jnp.float32, math.log(2.0), math.log(64.0))), 2.0, 64.0)
    step_length = jnp.clip(jax.random.uniform(key_of[4], (3,), jnp.float32, 0.1, 0.4), 0.1, 0.4)
    return dict(partial_grads=partial_grads, model=model, tilt=tilt, widths=widths, step_length=step_length)


def smoother(width_row):
    depths = jnp.arange(NZ, dtype=jnp.float32)
    offset = depths[:, None] - depths[None, :]
    kernel = jnp.exp(-offset * offset / (2.0 * width_row[:, None] * width_row[:, None]))
    return (kernel / jnp.sum(kernel, axis=1, keepdims=True)).astype(jnp.bfloat16)


def rotate(velocity, epsilon, delta, angle):
    squared = velocity * velocity
    along = squared * (1.0 + 2.0 * epsilon)
    normal = squared * (1.0 + 2.0 * delta)
    cosine = jnp.cos(angle)
    sine = jnp.sin(angle)
    first = along * cosine * cosine + squared * sine * sine
    second = along * sine * sine + squared * cosine * cosine
    third = (normal - squared) * sine * cosine
    return jnp.stack([first, second, third])


def average(padded):
    depth_cells = padded.shape[1] - 2
    x_cells = padded.shape[2] - 2
    weights = [0.25, 0.5, 0.25]
    total = jnp.zeros((padded.shape[0], depth_cells, x_cells, padded.shape[3]), jnp.float32)
    for shift_z in range(3):
        for shift_x in range(3):
            total = total + (weights[shift_z] * weights[shift_x]) * padded[:, shift_z:shift_z + depth_cells, shift_x:shift_x + x_cells, :]
    return total


def reference(partial_grads, model, tilt, widths, step_length):
    gradient = jnp.sum(partial_grads.astype(jnp.float32), axis=0).astype(jnp.bfloat16)
    smoothed_list = []
    for which in range(3):
        matrix = smoother(widths[which])
        flat = gradient[which].reshape(NZ, NX * NY)
        smoothed_list.append(jnp.dot(matrix, flat, preferred_element_type=jnp.float32).astype(jnp.bfloat16).reshape(NZ, NX, NY))
    smoothed = jnp.stack(smoothed_list)
    updated = model - step_length[:, None, None, None] * smoothed.astype(jnp.float32)
    rotated = rotate(updated[0], updated[1], updated[2], tilt)
    padded = jnp.pad(rotated, ((0, 0), (1, 1), (1, 1), (0, 0)))
    return average(padded)
```

```python
import functools

import jax
import jax.numpy as jnp
from jax import lax
from jax.experimental import pallas as pl
from jax.experimental.pallas import tpu as pltpu
from jax.sharding import PartitionSpec as P


INNER = 4
bf16 = jnp.bfloat16
f32 = jnp.float32


def call(kernel, scalars, args, in_specs, out_shapes, out_specs, scratch=(), grid=(1,)):
    return pl.pallas_call(
        kernel,
        grid_spec=pltpu.PrefetchScalarGridSpec(
            num_scalar_prefetch=1,
            grid=grid,
            in_specs=in_specs,
            out_specs=out_specs,
            scratch_shapes=scratch,
        ),
        out_shape=out_shapes,
    )(scalars, *args)


def whole(shape):
    return pl.BlockSpec(shape, lambda i, s: (0,) * len(shape))


def permute(value, axis, flip):
    count = lax.axis_size(axis)
    return lax.ppermute(value, axis, [(i, i ^ flip) for i in range(count)])


def shifted(value, axis, step):
    count = lax.axis_size(axis)
    pairs = [(i, i + step) for i in range(count) if 0 <= i + step < count]
    return lax.ppermute(value, axis, pairs)


def sum_body(scal, own, *refs, outer, x_group, others):
    received, outs, scratch = refs[:others], refs[others : others + outer], refs[-1]
    depth, x_local, lanes = own.shape[2:]
    total = own[0, 0].astype(f32)
    for ref in received:
        total = total + ref[...].astype(f32)
    scratch[...] = total.reshape(depth * x_local, lanes)
    for k in range(outer):
        for j in range(x_group):
            x = (scal[1] ^ k) * x_group + j
            outs[k][j] = scratch[pl.ds(x, depth, stride=x_local), :].astype(bf16)


def sum_and_split(scal, partial, p, received, outer, x_local):
    depth, y = partial.shape[2], partial.shape[4]
    x_group = x_local // outer
    block = 128
    out = jax.ShapeDtypeStruct((x_group, depth, y), bf16)
    return call(
        functools.partial(sum_body, outer=outer, x_group=x_group, others=len(received)),
        scal,
        (partial, *received),
        [pl.BlockSpec((1, 1, depth, x_local, block), lambda i, s: (0, p, 0, s[0], i))]
        + [pl.BlockSpec((depth, x_local, block), lambda i, s: (0, 0, i))] * len(received),
        [out] * outer,
        [pl.BlockSpec((x_group, depth, block), lambda i, s: (0, 0, i))] * outer,
        [pltpu.VMEM((depth * x_local, block), f32)],
        (y // block,),
    )


def join_body(scal, *refs, outer):
    parts, out = refs[:outer], refs[outer]
    depth = parts[0].shape[1]
    for k in range(outer):
        row = pl.multiple_of((scal[1] ^ k) * depth, depth)
        out[:, pl.ds(row, depth), :] = parts[k][...]


def join(scal, parts):
    outer = len(parts)
    x_group, depth, y = parts[0].shape
    shape = (x_group, outer * depth, y)
    return call(
        functools.partial(join_body, outer=outer),
        scal,
        parts,
        [whole(parts[0].shape)] * outer,
        jax.ShapeDtypeStruct(shape, bf16),
        whole(shape),
    )


def matrix_body(scal, width, out, *, outer, depth):
    p_count, _, rows, cols = out.shape
    row = lax.broadcasted_iota(jnp.int32, (rows, 1), 0)
    extra = row - outer * depth
    main = row < outer * depth
    group = jnp.where(main, row // depth, extra // 2)
    inside = jnp.where(main, row % depth, jnp.where(extra % 2 == 0, -1, depth))
    row_depth = (group * INNER + scal[2]) * depth + inside
    col = lax.broadcasted_iota(jnp.int32, (1, cols), 1)
    for p in range(p_count):
        w = width[p]
        scale = -1.0 / (2.0 * w * w)
        total = jnp.zeros((rows, 1), f32)
        kept = []
        for m in range(INNER):
            col_depth = (col // depth * INNER + (scal[2] ^ m)) * depth + col % depth
            offset = (row_depth - col_depth).astype(f32)
            kernel = jnp.exp(offset * offset * scale)
            total = total + jnp.sum(kernel, axis=1, keepdims=True)
            kept.append(kernel)
        for m in range(INNER):
            out[p, m] = (kept[m] / total).astype(bf16)


def matrices(scal, widths, outer, depth):
    p_count = widths.shape[0]
    split = (p_count, outer, INNER, depth)
    member = scal[2]
    before = jnp.concatenate([widths[:, :1], widths[:, :-1]], axis=1).reshape(split)
    after = jnp.concatenate([widths[:, 1:], widths[:, -1:]], axis=1).reshape(split)
    pick = lambda a: lax.dynamic_index_in_dim(a, member, 2, keepdims=False)
    main = pick(widths.reshape(split)).reshape(p_count, outer * depth)
    low = pick(before)[:, :, 0]
    high = pick(after)[:, :, depth - 1]
    edge = jnp.stack([low, high], axis=2).reshape(p_count, outer * 2)
    rows = outer * (depth + 2)
    width = jnp.concatenate([main, edge], axis=1)[:, :, None]
    shape = (p_count, INNER, rows, outer * depth)
    return call(
        functools.partial(matrix_body, outer=outer, depth=depth),
        scal,
        (width,),
        [whole(width.shape)],
        jax.ShapeDtypeStruct(shape, bf16),
        whole(shape),
    )


def smooth_body(scal, matrix, *refs, outer, depth):
    sources, outs, scratch, ends = refs[:INNER], refs[INNER : INNER + outer], refs[-2], refs[-1]
    x_group = sources[0].shape[0]
    for x in range(x_group):
        total = None
        for m in range(INNER):
            part = jnp.dot(matrix[0, m], sources[m][x], preferred_element_type=f32)
            total = part if total is None else total + part
        scratch[...] = total
        for k in range(outer):
            group = scal[1] ^ k
            row = pl.multiple_of(group * depth, depth)
            outs[k][x * depth : (x + 1) * depth, :] = scratch[pl.ds(row, depth), :].astype(bf16)
        for g in range(outer):
            base = outer * depth + 2 * g
            ends[g, 2 * x : 2 * x + 2, :] = total[base : base + 2, :]
    for k in range(outer):
        outs[k][x_group * depth :, :] = ends[scal[1] ^ k, 0 : 2 * x_group, :].astype(bf16)


def smooth(scal, matrix, p, sources, outer, depth):
    x_group, _, y = sources[0].shape
    rows = outer * (depth + 2)
    shape = (x_group * (depth + 2), y)
    return call(
        functools.partial(smooth_body, outer=outer, depth=depth),
        scal,
        (matrix, *sources),
        [pl.BlockSpec((1, INNER, rows, outer * depth), lambda i, s: (p, 0, 0, 0))]
        + [whole(sources[0].shape)] * INNER,
        [jax.ShapeDtypeStruct(shape, bf16)] * outer,
        [whole(shape)] * outer,
        [pltpu.VMEM((rows, y), f32), pltpu.VMEM((outer, -(-2 * x_group // 8) * 8, y), f32)],
    )


def edge_body(scal, *refs, outer, depth, x_group):
    parts, first, last = refs[:outer], refs[outer], refs[outer + 1]
    main = x_group * depth
    for k in range(outer):
        group = scal[1] ^ k

        @pl.when(group == 0)
        def _():
            first[0:depth, :] = parts[k][0:depth, :]
            first[depth : depth + 2, :] = parts[k][main : main + 2, :]

        @pl.when(group == outer - 1)
        def _():
            last[0:depth, :] = parts[k][main - depth : main, :]
            last[depth : depth + 2, :] = parts[k][main + 2 * x_group - 2 :, :]


def edges(scal, parts, depth):
    outer = len(parts)
    rows, y = parts[0].shape
    shape = (depth + 8, y)
    return call(
        functools.partial(edge_body, outer=outer, depth=depth, x_group=rows // (depth + 2)),
        scal,
        parts,
        [whole(parts[0].shape)] * outer,
        [jax.ShapeDtypeStruct(shape, bf16)] * 2,
        [whole(shape)] * 2,
    )


def plane_body(scal, model, tilt, xlow, xhigh, zlow, zhigh, out, border):
    x_local, depth = out.shape[1] - 2, out.shape[2]
    fields = out.shape[0]

    def put(x, rows, lowrow, highrow):
        for f in range(3):
            out[f, x] = rows[f]
            border[f, x, 0:1, :] = lowrow[f]
            border[f, x, 1:2, :] = highrow[f]
        for f, g in ((3, jnp.cos), (4, jnp.sin)):
            out[f, x] = g(2.0 * rows[3])
            border[f, x, 0:1, :] = g(2.0 * lowrow[3])
            border[f, x, 1:2, :] = g(2.0 * highrow[3])

    for x in range(x_local + 2):
        if x == 0:
            rows = [xlow[f] for f in range(4)]
        elif x == x_local + 1:
            rows = [xhigh[f] for f in range(4)]
        else:
            rows = [model[f, pl.ds(x - 1, depth, stride=x_local), :] for f in range(3)]
            rows.append(tilt[pl.ds(x - 1, depth, stride=x_local), :])
        put(
            x,
            rows,
            [zlow[f, x : x + 1, :] for f in range(4)],
            [zhigh[f, x : x + 1, :] for f in range(4)],
        )


def planes(scal, model, tilt):
    p_count, depth, x_local, y = model.shape
    fields = jnp.concatenate
    xfirst = jnp.concatenate([model[:, :, 0, :], tilt[None, :, 0, :]], axis=0)
    xlast = jnp.concatenate([model[:, :, -1, :], tilt[None, :, -1, :]], axis=0)
    xlow = shifted(xlast, "shot", 1)
    xhigh = shifted(xfirst, "shot", -1)
    zrow = lambda z: jnp.concatenate(
        [
            xlow[:, z, None, :],
            jnp.concatenate([model[:, z], tilt[None, z]], axis=0),
            xhigh[:, z, None, :],
        ],
        axis=1,
    )
    zlow = shifted(zrow(depth - 1), "slab", 1)
    zhigh = shifted(zrow(0), "slab", -1)
    block = 128
    main = jax.ShapeDtypeStruct((5, x_local + 2, depth, y), f32)
    border = jax.ShapeDtypeStruct((5, x_local + 2, 8, y), f32)
    lane3 = lambda i, s: (0, 0, i)
    return call(
        plane_body,
        scal,
        (
            model.reshape(p_count, depth * x_local, y),
            tilt.reshape(depth * x_local, y),
            xlow,
            xhigh,
            zlow,
            zhigh,
        ),
        [
            pl.BlockSpec((p_count, depth * x_local, block), lane3),
            pl.BlockSpec((depth * x_local, block), lambda i, s: (0, i)),
            pl.BlockSpec((4, depth, block), lane3),
            pl.BlockSpec((4, depth, block), lane3),
            pl.BlockSpec((4, x_local + 2, block), lane3),
            pl.BlockSpec((4, x_local + 2, block), lane3),
        ],
        [main, border],
        [
            pl.BlockSpec((5, x_local + 2, depth, block), lambda i, s: (0, 0, 0, i)),
            pl.BlockSpec((5, x_local + 2, 8, block), lambda i, s: (0, 0, 0, i)),
        ],
        grid=(y // block,),
    )


def final_body(scal, step, main, border, *refs, outer, x_group):
    out, smoothed, edge, fields = refs[-4:]
    parts = refs[: 3 * outer]
    sides = refs[3 * outer : 3 * outer + 6]
    x_local, depth, lanes = main.shape[1] - 2, main.shape[2], main.shape[3]
    for p in range(3):
        smoothed[p, 0] = sides[2 * p][0:depth, :].astype(f32)
        smoothed[p, x_local + 1] = sides[2 * p + 1][0:depth, :].astype(f32)
        edge[p, 0, 0:2, :] = sides[2 * p][depth : depth + 2, :].astype(f32)
        edge[p, x_local + 1, 0:2, :] = sides[2 * p + 1][depth : depth + 2, :].astype(f32)
        for k in range(outer):
            for j in range(x_group):
                x = (scal[1] ^ k) * x_group + j + 1
                ref = parts[p * outer + k]
                smoothed[p, x] = ref[j * depth : (j + 1) * depth, :].astype(f32)
                base = x_group * depth + 2 * j
                edge[p, x, 0:2, :] = ref[base : base + 2, :].astype(f32)

    def rotated(vp, eps, delta, cosine, sine):
        squared = vp * vp
        tilted = squared * eps
        turned = cosine * tilted
        return squared + tilted, turned, squared * delta * sine

    row = lax.broadcasted_iota(jnp.int32, (depth, lanes), 0)
    for x in range(x_local + 2):
        u = [main[p, x] - step[p] * smoothed[p, x] for p in range(3)]
        e = [border[p, x, 0:2, :] - step[p] * edge[p, x, 0:2, :] for p in range(3)]
        inner = rotated(*u, main[3, x], main[4, x])
        outerr = rotated(*e, border[3, x, 0:2, :], border[4, x, 0:2, :])
        for c in range(3):
            a = inner[c]
            low = jnp.where(scal[3] > 0, outerr[c][0:1, :], 0.0)
            high = jnp.where(scal[4] > 0, outerr[c][1:2, :], 0.0)
            up = jnp.where(row == 0, jnp.broadcast_to(low, a.shape), pltpu.roll(a, 1, 0))
            down = jnp.where(
                row == depth - 1, jnp.broadcast_to(high, a.shape), pltpu.roll(a, depth - 1, 0)
            )
            value = 0.5 * a + 0.25 * (up + down)
            if x == 0:
                value = jnp.where(scal[5] > 0, value, 0.0)
            if x == x_local + 1:
                value = jnp.where(scal[6] > 0, value, 0.0)
            fields[c, x] = value
    for x in range(x_local):
        mixed = [
            0.5 * fields[c, x + 1] + 0.25 * (fields[c, x] + fields[c, x + 2]) for c in range(3)
        ]
        out[0, pl.ds(x, depth, stride=x_local), :] = mixed[0] + mixed[1]
        out[1, pl.ds(x, depth, stride=x_local), :] = mixed[0] - mixed[1]
        out[2, pl.ds(x, depth, stride=x_local), :] = mixed[2]


def final(scal, step, main, border, parts, sides):
    outer = len(parts) // 3
    _, xs, depth, y = main.shape
    x_local = xs - 2
    block = 128
    lane4 = lambda i, s: (0, 0, 0, i)
    lane2 = lambda i, s: (0, i)
    return call(
        functools.partial(final_body, outer=outer, x_group=x_local // outer),
        scal,
        (step, main, border, *parts, *sides),
        [
            pl.BlockSpec(memory_space=pltpu.SMEM),
            pl.BlockSpec((5, xs, depth, block), lane4),
            pl.BlockSpec((5, xs, 8, block), lane4),
        ]
        + [pl.BlockSpec((a.shape[0], block), lane2) for a in (*parts, *sides)],
        jax.ShapeDtypeStruct((3, depth * x_local, y), f32),
        pl.BlockSpec((3, depth * x_local, block), lambda i, s: (0, 0, i)),
        [
            pltpu.VMEM((3, xs, depth, block), f32),
            pltpu.VMEM((3, xs, 8, block), f32),
            pltpu.VMEM((3, xs, depth, block), f32),
        ],
        (y // block,),
    )


def shards(partial_grads, model, tilt, widths, step_length):
    p_count, depth, x_local, y = model.shape
    shots = lax.axis_size("shot")
    slabs = lax.axis_size("slab")
    outer = slabs // INNER
    shot, slab = lax.axis_index("shot"), lax.axis_index("slab")
    scal = jnp.stack(
        [
            shot,
            slab // INNER,
            slab % INNER,
            jnp.where(slab > 0, 1, 0),
            jnp.where(slab < slabs - 1, 1, 0),
            jnp.where(shot > 0, 1, 0),
            jnp.where(shot < shots - 1, 1, 0),
        ]
    ).astype(jnp.int32)
    received = []
    for p in range(p_count):
        mine = partial_grads[0, p]
        received.append(
            [
                permute(
                    lax.dynamic_slice_in_dim(mine, (shot ^ s) * x_local, x_local, axis=1), "shot", s
                )
                for s in range(1, shots)
            ]
        )
    matrix = matrices(scal, widths, outer, depth)
    main, border = planes(scal, model, tilt)
    parts, sides = [], []
    for p in range(p_count):
        sends = sum_and_split(scal, partial_grads, p, received[p], outer, x_local)
        got = [sends[0]] + [permute(sends[k], "slab", k * INNER) for k in range(1, outer)]
        block = join(scal, got)
        far = permute(block, "slab", 2)
        near = permute(block, "slab", 1)
        both = permute(far, "slab", 1)
        backs = smooth(scal, matrix, p, (block, near, far, both), outer, depth)
        home = [backs[0]] + [permute(backs[k], "slab", k * INNER) for k in range(1, outer)]
        first, last = edges(scal, home, depth)
        parts += home
        sides += [shifted(last, "shot", 1), shifted(first, "shot", -1)]
    out = final(scal, step_length, main, border, parts, sides)
    return out.reshape(p_count, depth, x_local, y)


def solution(mesh):
    placed = (
        P("shot", None, "slab", None, None),
        P(None, "slab", "shot", None),
        P("slab", "shot", None),
        P(),
        P(),
    )
    return jax.shard_map(
        shards, mesh=mesh, in_specs=placed, out_specs=P(None, "slab", "shot", None), check_vma=False
    )
```
